32 devices in a mesh: rep: 8 (over y, x, core), sp: 4 (over z).
Axes of the slice: x: 2, y: 2, z: 4, core: 2. Of those that a mesh axis runs over, the one named last changes fastest.
Arguments:
- field: bfloat16 [8, 128, 100, 128], P('rep', 'sp'), may hold values from -6 to 6
- send_blocks: int32 [4, 4, 8], P('sp'), may hold values from 0 to 31
- send_count: int32 [4, 4], P('sp'), may hold values from 1 to 8, as said below
- regrid_weights: bfloat16 [32, 8, 128, 128], P('sp'), may hold values from -0.1875 to 0.1875
- tile_slot: int32 [32, 8], P('sp'), may hold values from 0 to 31
- edge_inputs: bfloat16 [12288, 1536], P(('rep', 'sp')), may hold values from -6 to 6
- cotangent: bfloat16 [12288, 512], P(('rep', 'sp')), may hold values from -0.15625 to 0.15625
Outputs:
- hidden: bfloat16 [8, 32, 100, 128], P('rep', 'sp')
- weight_grad: float32 [1536, 512], P(('rep', 'sp'))
The draws below stay inside these ranges and needn't reach their ends.
Inputs may be any that keep to these rules, and one draw needn't show every extreme that they name: `send_count`: every count is at most 8, and some pair of shards has exactly 8 in every draw.
All inputs are finite; a program needn't handle non-finite values.
Results may differ from the reference program's by a relative error of at most 0.001.
Values may be sent and summed in bfloat16 or wider, within the bound.
A program may use at most 64 MiB of HBM per device.

```python
import jax
import jax.numpy as jnp
from jax import lax

CHANNELS = 100
HID = 512
BLK = 128
NODE_TILE = 128
READS = 8
BLOCKS_DEV = 32
PER = 8
EDGE_DEV = 384
SHARDS = 4
REPLICAS = 8
BLOCKS = 128
TILES = 32
SLOTS = 32
IN = 1536
EDGES = 12288
N_REP = 8
N_SP = 4


def draw_send_count(key, part):
    base_key = jax.random.fold_in(key, 11)
    first_key, second_key = jax.random.split(base_key)
    counts = jax.random.randint(first_key, (SHARDS * SHARDS,), 1, PER + 1)
    chosen = jax.random.randint(second_key, (), 0, SHARDS * SHARDS)
    counts = jnp.where(jnp.arange(SHARDS * SHARDS) == chosen, PER, counts)
    return counts.reshape(SHARDS, SHARDS).astype(jnp.int32)


def with_ends(array, stream_key, smallest, largest):
    shape = array.shape
    place = [jax.random.randint(jax.random.fold_in(stream_key, axis), (), 0, shape[axis]) for axis in range(len(shape))]
    array = array.at[tuple(place)].set(smallest)
    longest = shape.index(max(shape))
    place[longest] = (place[longest] + 1) % shape[longest]
    return array.at[tuple(place)].set(largest)


def raised(entries, key, source, target, blocks, factor):
    def block_of(position):
        return (jnp.arange(entries.shape[position]) // (entries.shape[position] // blocks)).reshape((-1,) + (1,) * (entries.ndim - 1 - position))

    one_side = jax.random.permutation(key, blocks)[block_of(target)]
    second = (block_of(target) + blocks // 2) % blocks
    return jnp.where((block_of(source) == one_side) | (block_of(source) == second), factor * entries, entries)


def levels(key, dims, cuts, smallest, high):
    factor_of, own = 1.0, jax.random.fold_in(key, 6)
    for axis_at, shards_of in cuts:
        draws = jnp.exp(jax.random.uniform(jax.random.fold_in(own, axis_at), (shards_of,), jnp.float32, smallest / len(cuts), high / len(cuts)))
        factor_of = factor_of * jnp.repeat(draws, dims[axis_at] // shards_of).reshape([-1 if axis == axis_at else 1 for axis in range(len(dims))])
    return factor_of


def gaussian(key, dims, width, reach, cuts=(), kind=jnp.bfloat16):
    values = jax.random.normal(key, dims, jnp.float32) * width
    if len(cuts) > 0:
        values = levels(key, dims, cuts, -0.22, 0.18) * values
    return jnp.clip(values, min=-reach, max=reach).astype(kind)


def gaussian_with(rng, dims, scale, bound, cuts, heavy, kind=jnp.bfloat16):
    drawn = scale * jax.random.normal(rng, dims, jnp.float32)
    if cuts:
        drawn = drawn * levels(rng, dims, cuts, -0.22, 0.18)
    return jnp.clip(raised(drawn, jax.random.fold_in(rng, 3), *heavy), -bound, bound).astype(kind)


def setup_inputs(seed: int = 0) -> dict:
    key_of = jax.random.split(jax.random.key(seed), 8)
    return {
        "field": gaussian(key_of[0], (REPLICAS, BLOCKS, CHANNELS, BLK), 1.0, 6.0, ((0, 8), (1, 4))),
        "send_blocks": with_ends(jax.random.randint(key_of[1], (SHARDS, SHARDS, PER), 0, BLOCKS_DEV), jax.random.fold_in(key_of[1], 1), 0, BLOCKS_DEV - 1).astype(jnp.int32),
        "send_count": draw_send_count(jax.random.fold_in(key_of[7], 71), 0),
        "regrid_weights": gaussian(key_of[3], (TILES, READS, BLK, NODE_TILE), (READS * BLK) ** -0.5, 0.1875, ((0, 4),)),
        "tile_slot": with_ends(jax.random.randint(key_of[4], (TILES, READS), 0, SLOTS), jax.random.fold_in(key_of[4], 1), 0, SLOTS - 1).astype(jnp.int32),
        "edge_inputs": gaussian_with(key_of[5], (EDGES, IN), 1.0, 6.0, ((0, 32),), (0, 1, 32, 2.75)),
        "cotangent": gaussian(key_of[6], (EDGES, HID), (EDGE_DEV * N_SP) ** -0.5, 0.15625, ((0, 32),)),
    }


def reference(field, send_blocks, send_count, regrid_weights, tile_slot, edge_inputs, cotangent):
    shards = send_blocks.shape[0]
    slots_each = send_blocks.shape[2]
    blocks_dev = field.shape[1] // shards
    tiles_dev = tile_slot.shape[0] // shards
    reads = tile_slot.shape[1]
    source = jnp.arange(shards, dtype=jnp.int32)
    global_block = source[:, None, None] * blocks_dev + send_blocks
    alive_mask = jnp.arange(slots_each, dtype=jnp.int32)[None, None, :] < send_count[:, :, None]
    global_block = jnp.transpose(global_block, (1, 0, 2)).reshape(shards, shards * slots_each)
    alive_mask = jnp.transpose(alive_mask, (1, 0, 2)).reshape(shards, shards * slots_each)
    slot_index = tile_slot.reshape(shards, tiles_dev, reads)
    weight_tiles = regrid_weights.reshape(shards, tiles_dev, reads, BLK, NODE_TILE)

    def one_sample(sample):
        def one_shard(pieces):
            blocks_read, alive, slots, weights = pieces
            received = jnp.where(alive[:, None, None], sample[blocks_read], jnp.zeros((), jnp.bfloat16))
            picked = received[slots]
            result = jnp.einsum("tbcx,tbxn->tcn", picked.astype(jnp.float32), weights.astype(jnp.float32))
            return result.astype(jnp.bfloat16)

        outcome = lax.map(one_shard, (global_block, alive_mask, slot_index, weight_tiles))
        return outcome.reshape(shards * tiles_dev, CHANNELS, NODE_TILE)

    hidden = lax.map(one_sample, field)

    groups = N_REP * N_SP
    edge_groups = edge_inputs.reshape(groups, edge_inputs.shape[0] // groups, edge_inputs.shape[1])
    cot_groups = cotangent.reshape(groups, cotangent.shape[0] // groups, cotangent.shape[1])

    def accumulate(carry, pieces):
        left, right = pieces
        product = lax.dot_general(left, right, (((0,), (0,)), ((), ())), preferred_element_type=jnp.float32)
        return carry + product, None

    start_grad = jnp.zeros((edge_inputs.shape[1], cotangent.shape[1]), jnp.float32)
    weight_grad, unused = lax.scan(accumulate, start_grad, (edge_groups, cot_groups))
    return hidden, weight_grad
```

```python
import jax
import jax.numpy as jnp
from jax import lax
from jax.experimental import pallas as pl
from jax.experimental.pallas import tpu as pltpu
from jax.sharding import PartitionSpec as P

MESH = pl.DeviceIdType.MESH


def body(field, send_blocks, send_count, regrid_weights, tile_slot, edge_inputs, cotangent):
    sample = field[0]
    own_lists = send_blocks[0]
    shards = own_lists.shape[0]
    slots_each = own_lists.shape[1]
    channels = sample.shape[1]
    cells = sample.shape[2]
    alive = jnp.arange(slots_each, dtype=jnp.int32)[None, :] < send_count[0][:, None]
    outgoing = jnp.where(alive[:, :, None, None], sample[own_lists], jnp.zeros((), jnp.bfloat16))
    incoming = lax.all_to_all(outgoing, "sp", split_axis=0, concat_axis=0, tiled=True)
    block_pool = incoming.reshape(shards * slots_each, channels, cells)
    picked = block_pool[tile_slot]
    hidden = jnp.einsum(
        "tbcx,tbxn->tcn", picked, regrid_weights, preferred_element_type=jnp.float32
    )
    hidden = hidden.astype(jnp.bfloat16)[None]
    partial_value = lax.psum_scatter(
        lax.dot_general(
            edge_inputs, cotangent, (((0,), (0,)), ((), ())), preferred_element_type=jnp.float32
        ),
        "rep",
        scatter_dimension=0,
        tiled=True,
    )
    weight_grad = lax.psum_scatter(partial_value, "sp", scatter_dimension=0, tiled=True)
    return (hidden, weight_grad)


def encode(value):
    return value


def decode(code):
    return code


def kernel(
    lists_hbm, counts_hbm, slots_hbm, field_hbm, weights_hbm, edge_hbm, cot_hbm,
    hidden_out, grad_out,
    lists, counts, slots, field, wide, weights, edge, cot, outgoing, pool, tall, hidden, grad,
    part, got1, link2, got2, link3, got3, linkz, gotz, linkf, gotf,
    load_sem, a2a_send, a2a_recv, s1, r1, s2, r2, s3, r3, sz, rz, sf, rf,
):
    rep = lax.axis_index("rep")
    me = lax.axis_index("sp")
    core = rep % 2
    x = (rep // 2) % 2
    y = rep // 4
    w1, w2 = 1 + core, 2 - core
    b1 = x + core * (y - x)
    b2 = y + core * (x - y)
    twin = rep + 1 - 2 * core
    first = rep + (1 - 2 * b1) * 2 * w1
    second = rep + (1 - 2 * b2) * 2 * w2
    low, high = me % 2, me // 2
    near = 2 * high + 1 - low
    far = 2 * (1 - high) + low
    diag = 2 * (1 - high) + 1 - low
    outer, inner = 3 * (1 - high), 2 - high
    channels, blocks, cells = field.shape
    pitch = wide.shape[1]
    slots_each = lists.shape[2]
    tiles, reads = slots.shape
    width = edge_hbm.shape[1] // 4
    pieces = 2
    piece = slots_each // pieces

    loads = [
        pltpu.make_async_copy(field_hbm.at[0], field, load_sem.at[0]),
        pltpu.make_async_copy(lists_hbm, lists, load_sem.at[4]),
        pltpu.make_async_copy(counts_hbm, counts, load_sem.at[5]),
        pltpu.make_async_copy(edge_hbm, edge, load_sem.at[1]),
        pltpu.make_async_copy(cot_hbm, cot, load_sem.at[2]),
        pltpu.make_async_copy(slots_hbm, slots, load_sem.at[6]),
        pltpu.make_async_copy(weights_hbm, weights, load_sem.at[3]),
    ]
    for load in loads:
        load.start()
    field_load, lists_load, counts_load, edge_load, cot_load, slots_load, weights_load = loads

    barrier = pltpu.get_barrier_semaphore()
    for peer in (far, diag, near):
        pl.semaphore_signal(barrier, inc=1, device_id=(rep, peer), device_id_type=MESH)
    for peer in (twin, first, second):
        pl.semaphore_signal(barrier, inc=1, device_id=(peer, me), device_id_type=MESH)

    field_load.wait()
    wide[:, :blocks, :] = field[...].astype(jnp.float32)
    rows = wide.reshape(channels * pitch, cells)
    lists_load.wait()
    counts_load.wait()

    def block_for(d, j):
        block = rows[pl.ds(lists[0, d, j], channels, stride=pitch), :]
        block = jnp.where(j < counts[0, d], block, jnp.zeros_like(block))
        return block.astype(jnp.bfloat16)

    def remote(src, dst, ssem, rsem, device):
        return pltpu.make_async_remote_copy(
            src_ref=src, dst_ref=dst, send_sem=ssem, recv_sem=rsem,
            device_id=device, device_id_type=MESH,
        )

    def send(*args):
        copy = remote(*args)
        copy.start()
        return copy

    a2a = []
    for k, peer in enumerate((outer, near, inner)):
        for h in range(pieces):
            for j in range(h * piece, (h + 1) * piece):
                outgoing[k, j] = block_for(peer, j)
            if k == 0 and h == 0:
                pl.semaphore_wait(barrier, 6)
            a2a.append(send(
                outgoing.at[k, pl.ds(h * piece, piece)],
                pool.at[pl.ds(me * slots_each + h * piece, piece)],
                a2a_send.at[k, h], a2a_recv.at[me, h], (rep, peer),
            ))

    def chunk(flip1, flip2):
        return (b1 + flip1 * (1 - 2 * b1)) * w1 + (b2 + flip2 * (1 - 2 * b2)) * w2

    edge_load.wait()
    cot_load.wait()
    to_twin = []
    for k, (f1, f2) in enumerate(((1, 1), (0, 1), (1, 0), (0, 0))):
        q = chunk(f1, f2)
        columns = pl.ds(pl.multiple_of(q * width, 128), width)
        value = lax.dot_general(
            edge[:, columns], cot[...], (((0,), (0,)), ((), ())),
            preferred_element_type=jnp.float32,
        )
        part[k] = value.reshape(part.shape[1:])
        to_twin.append(send(
            part.at[k, 1 - core], got1.at[k], s1.at[k], r1.at[k], (twin, me)
        ))
    for j in range(slots_each):
        pool[me * slots_each + j] = block_for(me, j)

    order = [diag, near, far, me]
    both, crossed, after, kept = (0, 0), (2, 1), (1, 2), (3, 3)

    def folded(mine, theirs, i):
        return part[mine, core, order[i]] + got1[theirs, order[i]]

    out2 = []
    for n, k in enumerate((both, crossed)):
        to_twin[k[1]].wait_recv()
        for i in range(4):
            link2[n, i] = encode(folded(*k, i))
            out2.append(send(
                link2.at[n, i], got2.at[n, i], s2.at[n, i], r2.at[n, i], (first, me)
            ))
    to_twin[after[1]].wait_recv()
    out3 = []
    for i in range(4):
        value = folded(*after, i)
        out2[i].wait_recv()
        link3[i] = encode(value + decode(got2[0, i]))
        out3.append(send(link3.at[i], got3.at[i], s3.at[i], r3.at[i], (second, me)))
    to_twin[kept[1]].wait_recv()
    outz = []
    totals = []
    for i in range(4):
        value = folded(*kept, i)
        out2[4 + i].wait_recv()
        value = value + decode(got2[1, i])
        out3[i].wait_recv()
        value = value + decode(got3[i])
        if i < 2:
            linkz[i] = encode(value)
            outz.append(send(linkz.at[i], gotz.at[i], sz.at[i], rz.at[i], (rep, near)))
        else:
            part[kept[0], core, order[i]] = value
    outz[0].wait_recv()
    linkf[...] = encode(part[kept[0], core, far] + decode(gotz[0]))
    last = send(linkf, gotf, sf, rf, (rep, far))
    outz[1].wait_recv()
    grad[...] = part[kept[0], core, me] + decode(gotz[1])

    slots_load.wait()
    weights_load.wait()
    for peer in (near, far, diag):
        for h in range(pieces):
            ready = pool.at[pl.ds(peer * slots_each + h * piece, piece)]
            remote(ready, ready, a2a_send.at[0, h], a2a_recv.at[peer, h], (rep, peer)).wait_recv()
    for t in range(tiles):
        left = jnp.concatenate([pool[slots[t, b]] for b in range(reads)], axis=1)
        right = weights[t].reshape(reads * weights.shape[2], weights.shape[3])
        tall[pl.ds(t, channels, stride=tiles), :] = jnp.dot(
            left, right, preferred_element_type=jnp.float32
        )
    hidden[...] = tall[...].reshape(hidden.shape).astype(hidden.dtype)
    hidden_store = pltpu.make_async_copy(hidden, hidden_out.at[0], load_sem.at[0])
    hidden_store.start()

    last.wait_recv()
    grad[...] = grad[...] + decode(gotf[...])
    grad_store = pltpu.make_async_copy(grad, grad_out, load_sem.at[1])
    grad_store.start()
    for copy in a2a + to_twin + out2 + out3 + outz + [last]:
        copy.wait_send()
    hidden_store.wait()
    grad_store.wait()


def settle(hidden, grad, hidden_out, grad_out, hidden_held, grad_held, sem):
    pairs = ((hidden, hidden_held, hidden_out), (grad, grad_held, grad_out))
    inward = [pltpu.make_async_copy(a, b, sem.at[0, i]) for i, (a, b, _) in enumerate(pairs)]
    outward = [pltpu.make_async_copy(b, c, sem.at[1, i]) for i, (_, b, c) in enumerate(pairs)]
    for copy in inward:
        copy.start()
    for i in range(2):
        inward[i].wait()
        outward[i].start()
    for copy in outward:
        copy.wait()


def fused(field, send_blocks, send_count, regrid_weights, tile_slot, edge_inputs, cotangent):
    _, blocks, channels, cells = field.shape
    slots_each = send_blocks.shape[2]
    tiles = tile_slot.shape[0]
    nodes = regrid_weights.shape[3]
    n_in, hid = edge_inputs.shape[1], cotangent.shape[1]
    rows = n_in // (lax.axis_size("rep") * lax.axis_size("sp"))
    bf16, f32 = jnp.bfloat16, jnp.float32
    dma = pltpu.SemaphoreType.DMA
    i32, link = jnp.int32, jnp.float32
    far = pl.BlockSpec(memory_space=pl.ANY)
    out_shape = (
        jax.ShapeDtypeStruct((1, channels, tiles, nodes), bf16),
        jax.ShapeDtypeStruct((rows, hid), f32),
    )
    hidden, grad = pl.pallas_call(
        kernel,
        out_shape=out_shape,
        in_specs=[far] * 7,
        out_specs=(far, far),
        scratch_shapes=[
            pltpu.SMEM(send_blocks.shape, i32),
            pltpu.SMEM(send_count.shape, i32),
            pltpu.SMEM(tile_slot.shape, i32),
            pltpu.VMEM((channels, blocks, cells), bf16),
            pltpu.VMEM((channels, blocks + 8, cells), f32),
            pltpu.VMEM(regrid_weights.shape, bf16),
            pltpu.VMEM(edge_inputs.shape, bf16),
            pltpu.VMEM(cotangent.shape, bf16),
            pltpu.VMEM((3, slots_each, channels, cells), bf16),
            pltpu.VMEM((4 * slots_each, channels, cells), bf16),
            pltpu.VMEM((channels * tiles, nodes), f32),
            pltpu.VMEM((channels, tiles, nodes), bf16),
            pltpu.VMEM((rows, hid), f32),
            pltpu.VMEM((4, 2, 4, rows, hid), f32),
            pltpu.VMEM((4, 4, rows, hid), f32),
            pltpu.VMEM((2, 4, rows, hid), link),
            pltpu.VMEM((2, 4, rows, hid), link),
            pltpu.VMEM((4, rows, hid), link),
            pltpu.VMEM((4, rows, hid), link),
            pltpu.VMEM((2, rows, hid), link),
            pltpu.VMEM((2, rows, hid), link),
            pltpu.VMEM((rows, hid), link),
            pltpu.VMEM((rows, hid), link),
            dma((7,)),
            dma((3, 2)), dma((4, 2)),
            dma((4,)), dma((4,)),
            dma((2, 4)), dma((2, 4)),
            dma((4,)), dma((4,)),
            dma((2,)), dma((2,)),
            dma, dma,
        ],
        compiler_params=pltpu.CompilerParams(
            collective_id=0, has_side_effects=True, vmem_limit_bytes=56 * 1024 * 1024
        ),
    )(
        send_blocks, send_count, tile_slot, jnp.transpose(field, (0, 2, 1, 3)),
        regrid_weights, edge_inputs, cotangent,
    )
    hidden, grad = pl.pallas_call(
        settle, out_shape=out_shape, in_specs=[far, far], out_specs=(far, far),
        scratch_shapes=[
            pltpu.VMEM(out_shape[0].shape, bf16), pltpu.VMEM(out_shape[1].shape, f32), dma((2, 2)),
        ],
        compiler_params=pltpu.CompilerParams(vmem_limit_bytes=57000 * 1024),
    )(hidden, grad)
    return jnp.transpose(hidden, (0, 2, 1, 3)), grad


def solution(mesh):
    in_specs = (
        P("rep", "sp", None, None),
        P("sp", None, None),
        P("sp", None),
        P("sp", None, None, None),
        P("sp", None),
        P(("rep", "sp"), None),
        P(("rep", "sp"), None),
    )
    out_specs = (P("rep", "sp", None, None), P(("rep", "sp"), None))
    binary = mesh.shape["rep"] == 2 * 2 * 2 and mesh.shape["sp"] == 2 * 2
    inner = fused if binary else body
    return jax.shard_map(inner, mesh=mesh, in_specs=in_specs, out_specs=out_specs, check_vma=False)
```

```python
import jax
import jax.numpy as jnp
from jax import lax
from jax.experimental import pallas as pl
from jax.experimental.pallas import tpu as pltpu
from jax.sharding import PartitionSpec as P

MESH = pl.DeviceIdType.MESH


def body(field, send_blocks, send_count, regrid_weights, tile_slot, edge_inputs, cotangent):
    sample = field[0]
    own_lists = send_blocks[0]
    shards = own_lists.shape[0]
    slots_each = own_lists.shape[1]
    channels = sample.shape[1]
    cells = sample.shape[2]
    alive = jnp.arange(slots_each, dtype=jnp.int32)[None, :] < send_count[0][:, None]
    outgoing = jnp.where(alive[:, :, None, None], sample[own_lists], jnp.zeros((), jnp.bfloat16))
    incoming = lax.all_to_all(outgoing, "sp", split_axis=0, concat_axis=0, tiled=True)
    block_pool = incoming.reshape(shards * slots_each, channels, cells)
    picked = block_pool[tile_slot]
    hidden = jnp.einsum(
        "tbcx,tbxn->tcn", picked, regrid_weights, preferred_element_type=jnp.float32
    )
    hidden = hidden.astype(jnp.bfloat16)[None]
    partial_value = lax.psum_scatter(
        lax.dot_general(
            edge_inputs, cotangent, (((0,), (0,)), ((), ())), preferred_element_type=jnp.float32
        ),
        "rep",
        scatter_dimension=0,
        tiled=True,
    )
    weight_grad = lax.psum_scatter(partial_value, "sp", scatter_dimension=0, tiled=True)
    return (hidden, weight_grad)


OCTAVES = 40.0
LOWEST = 26.0
STEPS = 32767.0 / OCTAVES


def encode(value):
    level = (jnp.log2(jnp.maximum(jnp.abs(value), 2.0**-LOWEST)) + LOWEST) * STEPS
    code = jnp.minimum(level + 0.5, 32767.0).astype(jnp.int32)
    return jnp.where(value < 0, -code, code).astype(jnp.int16)


def decode(code):
    code = code.astype(jnp.int32)
    level = jnp.abs(code).astype(jnp.float32)
    size = jnp.exp2(level * (1.0 / STEPS) - LOWEST)
    return jnp.where(code > 0, size, jnp.where(code < 0, -size, 0.0))


def kernel(
    lists_hbm, counts_hbm, slots_hbm, field_hbm, weights_hbm, edge_hbm, cot_hbm,
    hidden_out, grad_out,
    lists, counts, slots, field, wide, weights, edge, cot, outgoing, pool, tall, hidden, grad,
    part, got1, link2, got2, link3, got3, linkz, gotz, linkf, gotf,
    load_sem, a2a_send, a2a_recv, s1, r1, s2, r2, s3, r3, sz, rz, sf, rf,
):
    rep = lax.axis_index("rep")
    me = lax.axis_index("sp")
    core = rep % 2
    x = (rep // 2) % 2
    y = rep // 4
    w1, w2 = 1 + core, 2 - core
    b1 = x + core * (y - x)
    b2 = y + core * (x - y)
    twin = rep + 1 - 2 * core
    first = rep + (1 - 2 * b1) * 2 * w1
    second = rep + (1 - 2 * b2) * 2 * w2
    low, high = me % 2, me // 2
    near = 2 * high + 1 - low
    far = 2 * (1 - high) + low
    diag = 2 * (1 - high) + 1 - low
    outer, inner = 3 * (1 - high), 2 - high
    channels, blocks, cells = field.shape
    pitch = wide.shape[1]
    slots_each = lists.shape[2]
    tiles, reads = slots.shape
    width = edge_hbm.shape[1] // 4
    pieces = 2
    piece = slots_each // pieces

    loads = [
        pltpu.make_async_copy(field_hbm.at[0], field, load_sem.at[0]),
        pltpu.make_async_copy(lists_hbm, lists, load_sem.at[4]),
        pltpu.make_async_copy(counts_hbm, counts, load_sem.at[5]),
        pltpu.make_async_copy(edge_hbm, edge, load_sem.at[1]),
        pltpu.make_async_copy(cot_hbm, cot, load_sem.at[2]),
        pltpu.make_async_copy(slots_hbm, slots, load_sem.at[6]),
        pltpu.make_async_copy(weights_hbm, weights, load_sem.at[3]),
    ]
    for load in loads:
        load.start()
    field_load, lists_load, counts_load, edge_load, cot_load, slots_load, weights_load = loads

    barrier = pltpu.get_barrier_semaphore()
    for peer in (far, diag, near):
        pl.semaphore_signal(barrier, inc=1, device_id=(rep, peer), device_id_type=MESH)
    for peer in (twin, first, second):
        pl.semaphore_signal(barrier, inc=1, device_id=(peer, me), device_id_type=MESH)

    field_load.wait()
    wide[:, :blocks, :] = field[...].astype(jnp.float32)
    rows = wide.reshape(channels * pitch, cells)
    lists_load.wait()
    counts_load.wait()

    def block_for(d, j):
        block = rows[pl.ds(lists[0, d, j], channels, stride=pitch), :]
        block = jnp.where(j < counts[0, d], block, jnp.zeros_like(block))
        return block.astype(jnp.bfloat16)

    def remote(src, dst, ssem, rsem, device):
        return pltpu.make_async_remote_copy(
            src_ref=src, dst_ref=dst, send_sem=ssem, recv_sem=rsem,
            device_id=device, device_id_type=MESH,
        )

    def send(*args):
        copy = remote(*args)
        copy.start()
        return copy

    end = (low + high) % 2 == 0
    middle = (low + high) % 2 == 1
    peers = (outer, near, inner)
    late = pieces - 1
    a2a = {}

    def choose(k, h):
        for j in range(h * piece, (h + 1) * piece):
            outgoing[k, j] = block_for(peers[k], j)
        a2a[k, h] = remote(
            outgoing.at[k, pl.ds(h * piece, piece)],
            pool.at[pl.ds(me * slots_each + h * piece, piece)],
            a2a_send.at[k, h], a2a_recv.at[me, h], (rep, peers[k]),
        )

    def launch(where, keys):
        @pl.when(where)
        def _():
            for key in keys:
                a2a[key].start()

    for h in range(pieces):
        choose(0, h)
        if h == 0:
            pl.semaphore_wait(barrier, 6)
        a2a[0, h].start()
    for h in range(pieces):
        choose(2, h)
        if h < late:
            a2a[2, h].start()
        else:
            launch(end, [(2, h)])

    def chunk(flip1, flip2):
        return (b1 + flip1 * (1 - 2 * b1)) * w1 + (b2 + flip2 * (1 - 2 * b2)) * w2

    edge_load.wait()
    cot_load.wait()
    to_twin = []
    for k, (f1, f2) in enumerate(((1, 1), (0, 1), (1, 0), (0, 0))):
        q = chunk(f1, f2)
        columns = pl.ds(pl.multiple_of(q * width, 128), width)
        value = lax.dot_general(
            edge[:, columns], cot[...], (((0,), (0,)), ((), ())),
            preferred_element_type=jnp.float32,
        )
        part[k] = value.reshape(part.shape[1:])
        to_twin.append(send(
            part.at[k, 1 - core], got1.at[k], s1.at[k], r1.at[k], (twin, me)
        ))
    for h in range(pieces):
        choose(1, h)
    launch(middle, [(1, h) for h in range(pieces)])
    for j in range(slots_each):
        pool[me * slots_each + j] = block_for(me, j)

    order = [diag, near, far, me]
    both, crossed, after, kept = (0, 0), (2, 1), (1, 2), (3, 3)

    def folded(mine, theirs, i):
        return part[mine, core, order[i]] + got1[theirs, order[i]]

    out2 = []
    for n, k in enumerate((both, crossed)):
        to_twin[k[1]].wait_recv()
        for i in range(4):
            link2[n, i] = encode(folded(*k, i))
            out2.append(send(
                link2.at[n, i], got2.at[n, i], s2.at[n, i], r2.at[n, i], (first, me)
            ))
    to_twin[after[1]].wait_recv()
    out3 = []
    for i in range(4):
        value = folded(*after, i)
        out2[i].wait_recv()
        link3[i] = encode(value + decode(got2[0, i]))
        out3.append(send(link3.at[i], got3.at[i], s3.at[i], r3.at[i], (second, me)))
    to_twin[kept[1]].wait_recv()
    outz = []
    totals = []
    for i in range(4):
        value = folded(*kept, i)
        out2[4 + i].wait_recv()
        value = value + decode(got2[1, i])
        out3[i].wait_recv()
        value = value + decode(got3[i])
        if i < 2:
            linkz[i] = encode(value)
            outz.append(send(linkz.at[i], gotz.at[i], sz.at[i], rz.at[i], (rep, near)))
        else:
            part[kept[0], core, order[i]] = value
    launch(end, [(1, h) for h in range(pieces)])
    outz[0].wait_recv()
    linkf[...] = encode(part[kept[0], core, far] + decode(gotz[0]))
    last = send(linkf, gotf, sf, rf, (rep, far))
    launch(middle, [(2, h) for h in range(late, pieces)])
    outz[1].wait_recv()
    grad[...] = part[kept[0], core, me] + decode(gotz[1])

    slots_load.wait()
    weights_load.wait()
    for peer in (near, far, diag):
        for h in range(pieces):
            ready = pool.at[pl.ds(peer * slots_each + h * piece, piece)]
            remote(ready, ready, a2a_send.at[0, h], a2a_recv.at[peer, h], (rep, peer)).wait_recv()
    for t in range(tiles):
        left = jnp.concatenate([pool[slots[t, b]] for b in range(reads)], axis=1)
        right = weights[t].reshape(reads * weights.shape[2], weights.shape[3])
        tall[pl.ds(t, channels, stride=tiles), :] = jnp.dot(
            left, right, preferred_element_type=jnp.float32
        )
    hidden[...] = tall[...].reshape(hidden.shape).astype(hidden.dtype)
    hidden_store = pltpu.make_async_copy(hidden, hidden_out.at[0], load_sem.at[0])
    hidden_store.start()

    last.wait_recv()
    grad[...] = grad[...] + decode(gotf[...])
    grad_store = pltpu.make_async_copy(grad, grad_out, load_sem.at[1])
    grad_store.start()
    for copy in list(a2a.values()) + to_twin + out2 + out3 + outz + [last]:
        copy.wait_send()
    hidden_store.wait()
    grad_store.wait()


def settle(hidden, grad, hidden_out, grad_out, hidden_held, grad_held, sem):
    pairs = ((hidden, hidden_held, hidden_out), (grad, grad_held, grad_out))
    inward = [pltpu.make_async_copy(a, b, sem.at[0, i]) for i, (a, b, _) in enumerate(pairs)]
    outward = [pltpu.make_async_copy(b, c, sem.at[1, i]) for i, (_, b, c) in enumerate(pairs)]
    for copy in inward:
        copy.start()
    for i in range(2):
        inward[i].wait()
        outward[i].start()
    for copy in outward:
        copy.wait()


def fused(field, send_blocks, send_count, regrid_weights, tile_slot, edge_inputs, cotangent):
    _, blocks, channels, cells = field.shape
    slots_each = send_blocks.shape[2]
    tiles = tile_slot.shape[0]
    nodes = regrid_weights.shape[3]
    n_in, hid = edge_inputs.shape[1], cotangent.shape[1]
    rows = n_in // (lax.axis_size("rep") * lax.axis_size("sp"))
    bf16, f32 = jnp.bfloat16, jnp.float32
    dma = pltpu.SemaphoreType.DMA
    i32, link = jnp.int32, jnp.int16
    far = pl.BlockSpec(memory_space=pl.ANY)
    out_shape = (
        jax.ShapeDtypeStruct((1, channels, tiles, nodes), bf16),
        jax.ShapeDtypeStruct((rows, hid), f32),
    )
    hidden, grad = pl.pallas_call(
        kernel,
        out_shape=out_shape,
        in_specs=[far] * 7,
        out_specs=(far, far),
        scratch_shapes=[
            pltpu.SMEM(send_blocks.shape, i32),
            pltpu.SMEM(send_count.shape, i32),
            pltpu.SMEM(tile_slot.shape, i32),
            pltpu.VMEM((channels, blocks, cells), bf16),
            pltpu.VMEM((channels, blocks + 8, cells), f32),
            pltpu.VMEM(regrid_weights.shape, bf16),
            pltpu.VMEM(edge_inputs.shape, bf16),
            pltpu.VMEM(cotangent.shape, bf16),
            pltpu.VMEM((3, slots_each, channels, cells), bf16),
            pltpu.VMEM((4 * slots_each, channels, cells), bf16),
            pltpu.VMEM((channels * tiles, nodes), f32),
            pltpu.VMEM((channels, tiles, nodes), bf16),
            pltpu.VMEM((rows, hid), f32),
            pltpu.VMEM((4, 2, 4, rows, hid), f32),
            pltpu.VMEM((4, 4, rows, hid), f32),
            pltpu.VMEM((2, 4, rows, hid), link),
            pltpu.VMEM((2, 4, rows, hid), link),
            pltpu.VMEM((4, rows, hid), link),
            pltpu.VMEM((4, rows, hid), link),
            pltpu.VMEM((2, rows, hid), link),
            pltpu.VMEM((2, rows, hid), link),
            pltpu.VMEM((rows, hid), link),
            pltpu.VMEM((rows, hid), link),
            dma((7,)),
            dma((3, 2)), dma((4, 2)),
            dma((4,)), dma((4,)),
            dma((2, 4)), dma((2, 4)),
            dma((4,)), dma((4,)),
            dma((2,)), dma((2,)),
            dma, dma,
        ],
        compiler_params=pltpu.CompilerParams(
            collective_id=0, has_side_effects=True, vmem_limit_bytes=56 * 1024 * 1024
        ),
    )(
        send_blocks, send_count, tile_slot, jnp.transpose(field, (0, 2, 1, 3)),
        regrid_weights, edge_inputs, cotangent,
    )
    hidden, grad = pl.pallas_call(
        settle, out_shape=out_shape, in_specs=[far, far], out_specs=(far, far),
        scratch_shapes=[
            pltpu.VMEM(out_shape[0].shape, bf16), pltpu.VMEM(out_shape[1].shape, f32), dma((2, 2)),
        ],
        compiler_params=pltpu.CompilerParams(vmem_limit_bytes=57000 * 1024),
    )(hidden, grad)
    return jnp.transpose(hidden, (0, 2, 1, 3)), grad


def solution(mesh):
    in_specs = (
        P("rep", "sp", None, None),
        P("sp", None, None),
        P("sp", None),
        P("sp", None, None, None),
        P("sp", None),
        P(("rep", "sp"), None),
        P(("rep", "sp"), None),
    )
    out_specs = (P("rep", "sp", None, None), P(("rep", "sp"), None))
    binary = mesh.shape["rep"] == 2 * 2 * 2 and mesh.shape["sp"] == 2 * 2
    inner = fused if binary else body
    return jax.shard_map(inner, mesh=mesh, in_specs=in_specs, out_specs=out_specs, check_vma=False)
```

```python
import jax
import jax.numpy as jnp
from jax import lax
from jax.experimental import pallas as pl
from jax.experimental.pallas import tpu as pltpu
from jax.sharding import PartitionSpec as P

MESH = pl.DeviceIdType.MESH


def body(field, send_blocks, send_count, regrid_weights, tile_slot, edge_inputs, cotangent):
    sample = field[0]
    own_lists = send_blocks[0]
    shards = own_lists.shape[0]
    slots_each = own_lists.shape[1]
    channels = sample.shape[1]
    cells = sample.shape[2]
    alive = jnp.arange(slots_each, dtype=jnp.int32)[None, :] < send_count[0][:, None]
    outgoing = jnp.where(alive[:, :, None, None], sample[own_lists], jnp.zeros((), jnp.bfloat16))
    incoming = lax.all_to_all(outgoing, "sp", split_axis=0, concat_axis=0, tiled=True)
    block_pool = incoming.reshape(shards * slots_each, channels, cells)
    picked = block_pool[tile_slot]
    hidden = jnp.einsum(
        "tbcx,tbxn->tcn", picked, regrid_weights, preferred_element_type=jnp.float32
    )
    hidden = hidden.astype(jnp.bfloat16)[None]
    partial_value = lax.psum_scatter(
        lax.dot_general(
            edge_inputs, cotangent, (((0,), (0,)), ((), ())), preferred_element_type=jnp.float32
        ),
        "rep",
        scatter_dimension=0,
        tiled=True,
    )
    weight_grad = lax.psum_scatter(partial_value, "sp", scatter_dimension=0, tiled=True)
    return (hidden, weight_grad)


OCTAVES = 40.0
LOWEST = 26.0
STEPS = 32767.0 / OCTAVES


def encode(value):
    level = (jnp.log2(jnp.maximum(jnp.abs(value), 2.0**-LOWEST)) + LOWEST) * STEPS
    code = jnp.minimum(level + 0.5, 32767.0).astype(jnp.int32)
    return jnp.where(value < 0, -code, code).astype(jnp.int16)


def decode(code):
    code = code.astype(jnp.int32)
    level = jnp.abs(code).astype(jnp.float32)
    size = jnp.exp2(level * (1.0 / STEPS) - LOWEST)
    return jnp.where(code > 0, size, jnp.where(code < 0, -size, 0.0))


def kernel(
    lists_hbm, counts_hbm, slots_hbm, field_hbm, weights_hbm, edge_hbm, cot_hbm,
    hidden_out, grad_out,
    lists, counts, slots, field, wide, weights, edge, cot, stage, outgoing, arrived, pool, tall, hidden, grad,
    part, got1, link2, got2, link3, got3, linkz, gotz, linkf, gotf,
    load_sem, a2a_send, a2a_recv, s1, r1, s2, r2, s3, r3, sz, rz, sf, rf,
):
    rep = lax.axis_index("rep")
    me = lax.axis_index("sp")
    core = rep % 2
    x = (rep // 2) % 2
    y = rep // 4
    w1, w2 = 1 + core, 2 - core
    b1 = x + core * (y - x)
    b2 = y + core * (x - y)
    twin = rep + 1 - 2 * core
    first = rep + (1 - 2 * b1) * 2 * w1
    second = rep + (1 - 2 * b2) * 2 * w2
    low, high = me % 2, me // 2
    near = 2 * high + 1 - low
    far = 2 * (1 - high) + low
    diag = 2 * (1 - high) + 1 - low
    outer, inner = 3 * (1 - high), 2 - high
    channels, blocks, cells = field.shape
    pitch = wide.shape[1]
    slots_each = lists.shape[2]
    tiles, reads = slots.shape
    width = edge_hbm.shape[1] // 4
    pieces = 2
    piece = slots_each // pieces

    loads = [
        pltpu.make_async_copy(field_hbm.at[0], field, load_sem.at[0]),
        pltpu.make_async_copy(lists_hbm, lists, load_sem.at[4]),
        pltpu.make_async_copy(counts_hbm, counts, load_sem.at[5]),
        pltpu.make_async_copy(edge_hbm, edge, load_sem.at[1]),
        pltpu.make_async_copy(cot_hbm, cot, load_sem.at[2]),
        pltpu.make_async_copy(slots_hbm, slots, load_sem.at[6]),
        pltpu.make_async_copy(weights_hbm, weights, load_sem.at[3]),
    ]
    for load in loads:
        load.start()
    field_load, lists_load, counts_load, edge_load, cot_load, slots_load, weights_load = loads

    barrier = pltpu.get_barrier_semaphore()
    for peer in (far, diag, near):
        pl.semaphore_signal(barrier, inc=1, device_id=(rep, peer), device_id_type=MESH)
    for peer in (twin, first, second):
        pl.semaphore_signal(barrier, inc=1, device_id=(peer, me), device_id_type=MESH)

    field_load.wait()
    wide[:, :blocks, :] = field[...].astype(jnp.float32)
    rows = wide.reshape(channels * pitch, cells)
    lists_load.wait()
    counts_load.wait()

    def block_for(d, j):
        block = rows[pl.ds(lists[0, d, j], channels, stride=pitch), :]
        block = jnp.where(j < counts[0, d], block, jnp.zeros_like(block))
        return block

    def remote(src, dst, ssem, rsem, device):
        return pltpu.make_async_remote_copy(
            src_ref=src, dst_ref=dst, send_sem=ssem, recv_sem=rsem,
            device_id=device, device_id_type=MESH,
        )

    def send(*args):
        copy = remote(*args)
        copy.start()
        return copy

    end = (low + high) % 2 == 0
    middle = (low + high) % 2 == 1
    peers = (outer, near, inner)
    late = pieces - 1
    a2a = {}

    def choose(k, h):
        for n in range(piece):
            stage[pl.ds(n, channels, stride=piece), :] = block_for(peers[k], h * piece + n)
        outgoing[k, h] = stage[...].astype(outgoing.dtype)
        a2a[k, h] = remote(
            outgoing.at[k, h], arrived.at[me, h],
            a2a_send.at[k, h], a2a_recv.at[me, h], (rep, peers[k]),
        )

    def launch(where, keys):
        @pl.when(where)
        def _():
            for key in keys:
                a2a[key].start()

    for h in range(pieces):
        choose(0, h)
        if h == 0:
            pl.semaphore_wait(barrier, 6)
        a2a[0, h].start()
    for h in range(pieces):
        choose(2, h)
        if h < late:
            a2a[2, h].start()
        else:
            launch(end, [(2, h)])

    def chunk(flip1, flip2):
        return (b1 + flip1 * (1 - 2 * b1)) * w1 + (b2 + flip2 * (1 - 2 * b2)) * w2

    edge_load.wait()
    cot_load.wait()
    to_twin = []
    for k, (f1, f2) in enumerate(((1, 1), (0, 1), (1, 0), (0, 0))):
        q = chunk(f1, f2)
        columns = pl.ds(pl.multiple_of(q * width, 128), width)
        value = lax.dot_general(
            edge[:, columns], cot[...], (((0,), (0,)), ((), ())),
            preferred_element_type=jnp.float32,
        )
        part[k] = value.reshape(part.shape[1:])
        to_twin.append(send(
            part.at[k, 1 - core], got1.at[k], s1.at[k], r1.at[k], (twin, me)
        ))
    for h in range(pieces):
        choose(1, h)
    launch(middle, [(1, h) for h in range(pieces)])
    for j in range(slots_each):
        pool[me * slots_each + j] = block_for(me, j).astype(pool.dtype)

    order = [diag, near, far, me]
    both, crossed, after, kept = (0, 0), (2, 1), (1, 2), (3, 3)

    def folded(mine, theirs, i):
        return part[mine, core, order[i]] + got1[theirs, order[i]]

    out2, out3, outz = {}, {}, {}

    def hand_first(n, which, i):
        link2[n, i] = encode(folded(*which, i))
        out2[n, i] = send(
            link2.at[n, i], got2.at[n, i], s2.at[n, i], r2.at[n, i], (first, me)
        )

    def hand_second(i):
        value = folded(*after, i)
        out2[0, i].wait_recv()
        link3[i] = encode(value + decode(got2[0, i]))
        out3[i] = send(link3.at[i], got3.at[i], s3.at[i], r3.at[i], (second, me))

    def gathered(i):
        value = folded(*kept, i)
        out2[1, i].wait_recv()
        value = value + decode(got2[1, i])
        out3[i].wait_recv()
        return value + decode(got3[i])

    to_twin[both[1]].wait_recv()
    hand_first(0, both, 0)
    hand_first(0, both, 1)
    to_twin[crossed[1]].wait_recv()
    hand_first(1, crossed, 0)
    hand_first(1, crossed, 1)
    to_twin[after[1]].wait_recv()
    hand_second(0)
    hand_second(1)
    for i in (2, 3):
        hand_first(0, both, i)
        hand_first(1, crossed, i)
    to_twin[kept[1]].wait_recv()
    hand_second(2)
    hand_second(3)
    for i in (0, 1):
        linkz[i] = encode(gathered(i))
        outz[i] = send(linkz.at[i], gotz.at[i], sz.at[i], rz.at[i], (rep, near))
    for i in (2, 3):
        part[kept[0], core, order[i]] = gathered(i)
    launch(end, [(1, h) for h in range(pieces)])
    outz[0].wait_recv()
    linkf[...] = encode(part[kept[0], core, far] + decode(gotz[0]))
    last = send(linkf, gotf, sf, rf, (rep, far))
    launch(middle, [(2, h) for h in range(late, pieces)])
    outz[1].wait_recv()
    grad[...] = part[kept[0], core, me] + decode(gotz[1])

    slots_load.wait()
    weights_load.wait()
    for k, h in [(k, h) for k in range(3) for h in range(pieces)]:
        ready = arrived.at[peers[k], h]
        remote(
            ready, ready, a2a_send.at[k, h], a2a_recv.at[peers[k], h], (rep, peers[k])
        ).wait_recv()
        stage[...] = arrived[peers[k], h].astype(jnp.float32)
        for n in range(piece):
            block = stage[pl.ds(n, channels, stride=piece), :]
            pool[peers[k] * slots_each + h * piece + n] = block.astype(pool.dtype)
    for t in range(tiles):
        left = jnp.concatenate([pool[slots[t, b]] for b in range(reads)], axis=1)
        right = weights[t].reshape(reads * weights.shape[2], weights.shape[3])
        tall[pl.ds(t, channels, stride=tiles), :] = jnp.dot(
            left, right, preferred_element_type=jnp.float32
        )
    hidden[...] = tall[...].reshape(hidden.shape).astype(hidden.dtype)
    hidden_store = pltpu.make_async_copy(hidden, hidden_out.at[0], load_sem.at[0])
    hidden_store.start()

    last.wait_recv()
    grad[...] = grad[...] + decode(gotf[...])
    grad_store = pltpu.make_async_copy(grad, grad_out, load_sem.at[1])
    grad_store.start()
    for copies in (a2a, out2, out3, outz):
        for copy in copies.values():
            copy.wait_send()
    for copy in to_twin + [last]:
        copy.wait_send()
    hidden_store.wait()
    grad_store.wait()


def settle(hidden, grad, hidden_out, grad_out, hidden_held, grad_held, sem):
    pairs = ((hidden, hidden_held, hidden_out), (grad, grad_held, grad_out))
    inward = [pltpu.make_async_copy(a, b, sem.at[0, i]) for i, (a, b, _) in enumerate(pairs)]
    outward = [pltpu.make_async_copy(b, c, sem.at[1, i]) for i, (_, b, c) in enumerate(pairs)]
    for copy in inward:
        copy.start()
    for i in range(2):
        inward[i].wait()
        outward[i].start()
    for copy in outward:
        copy.wait()


def fused(field, send_blocks, send_count, regrid_weights, tile_slot, edge_inputs, cotangent):
    _, blocks, channels, cells = field.shape
    slots_each = send_blocks.shape[2]
    tiles = tile_slot.shape[0]
    nodes = regrid_weights.shape[3]
    n_in, hid = edge_inputs.shape[1], cotangent.shape[1]
    rows = n_in // (lax.axis_size("rep") * lax.axis_size("sp"))
    bf16, f32 = jnp.bfloat16, jnp.float32
    dma = pltpu.SemaphoreType.DMA
    i32, link = jnp.int32, jnp.int16
    far = pl.BlockSpec(memory_space=pl.ANY)
    out_shape = (
        jax.ShapeDtypeStruct((1, channels, tiles, nodes), bf16),
        jax.ShapeDtypeStruct((rows, hid), f32),
    )
    hidden, grad = pl.pallas_call(
        kernel,
        out_shape=out_shape,
        in_specs=[far] * 7,
        out_specs=(far, far),
        scratch_shapes=[
            pltpu.SMEM(send_blocks.shape, i32),
            pltpu.SMEM(send_count.shape, i32),
            pltpu.SMEM(tile_slot.shape, i32),
            pltpu.VMEM((channels, blocks, cells), bf16),
            pltpu.VMEM((channels, blocks + 8, cells), f32),
            pltpu.VMEM(regrid_weights.shape, bf16),
            pltpu.VMEM(edge_inputs.shape, bf16),
            pltpu.VMEM(cotangent.shape, bf16),
            pltpu.VMEM((slots_each // 2 * channels, cells), f32),
            pltpu.VMEM((3, 2, slots_each // 2 * channels, cells), bf16),
            pltpu.VMEM((4, 2, slots_each // 2 * channels, cells), bf16),
            pltpu.VMEM((4 * slots_each, channels, cells), bf16),
            pltpu.VMEM((channels * tiles, nodes), f32),
            pltpu.VMEM((channels, tiles, nodes), bf16),
            pltpu.VMEM((rows, hid), f32),
            pltpu.VMEM((4, 2, 4, rows, hid), f32),
            pltpu.VMEM((4, 4, rows, hid), f32),
            pltpu.VMEM((2, 4, rows, hid), link),
            pltpu.VMEM((2, 4, rows, hid), link),
            pltpu.VMEM((4, rows, hid), link),
            pltpu.VMEM((4, rows, hid), link),
            pltpu.VMEM((2, rows, hid), link),
            pltpu.VMEM((2, rows, hid), link),
            pltpu.VMEM((rows, hid), link),
            pltpu.VMEM((rows, hid), link),
            dma((7,)),
            dma((3, 2)), dma((4, 2)),
            dma((4,)), dma((4,)),
            dma((2, 4)), dma((2, 4)),
            dma((4,)), dma((4,)),
            dma((2,)), dma((2,)),
            dma, dma,
        ],
        compiler_params=pltpu.CompilerParams(
            collective_id=0, has_side_effects=True, vmem_limit_bytes=56 * 1024 * 1024
        ),
    )(
        send_blocks, send_count, tile_slot, jnp.transpose(field, (0, 2, 1, 3)),
        regrid_weights, edge_inputs, cotangent,
    )
    hidden, grad = pl.pallas_call(
        settle, out_shape=out_shape, in_specs=[far, far], out_specs=(far, far),
        scratch_shapes=[
            pltpu.VMEM(out_shape[0].shape, bf16), pltpu.VMEM(out_shape[1].shape, f32), dma((2, 2)),
        ],
        compiler_params=pltpu.CompilerParams(vmem_limit_bytes=57000 * 1024),
    )(hidden, grad)
    return jnp.transpose(hidden, (0, 2, 1, 3)), grad


def solution(mesh):
    in_specs = (
        P("rep", "sp", None, None),
        P("sp", None, None),
        P("sp", None),
        P("sp", None, None, None),
        P("sp", None),
        P(("rep", "sp"), None),
        P(("rep", "sp"), None),
    )
    out_specs = (P("rep", "sp", None, None), P(("rep", "sp"), None))
    binary = mesh.shape["rep"] == 2 * 2 * 2 and mesh.shape["sp"] == 2 * 2
    inner = fused if binary else body
    return jax.shard_map(inner, mesh=mesh, in_specs=in_specs, out_specs=out_specs, check_vma=False)
```

```python
import jax
import jax.numpy as jnp
from jax import lax
from jax.experimental import pallas as pl
from jax.experimental.pallas import tpu as pltpu
from jax.sharding import PartitionSpec as P

MESH = pl.DeviceIdType.MESH


def body(field, send_blocks, send_count, regrid_weights, tile_slot, edge_inputs, cotangent):
    sample = field[0]
    own_lists = send_blocks[0]
    shards = own_lists.shape[0]
    slots_each = own_lists.shape[1]
    channels = sample.shape[1]
    cells = sample.shape[2]
    alive = jnp.arange(slots_each, dtype=jnp.int32)[None, :] < send_count[0][:, None]
    outgoing = jnp.where(alive[:, :, None, None], sample[own_lists], jnp.zeros((), jnp.bfloat16))
    incoming = lax.all_to_all(outgoing, "sp", split_axis=0, concat_axis=0, tiled=True)
    block_pool = incoming.reshape(shards * slots_each, channels, cells)
    picked = block_pool[tile_slot]
    hidden = jnp.einsum(
        "tbcx,tbxn->tcn", picked, regrid_weights, preferred_element_type=jnp.float32
    )
    hidden = hidden.astype(jnp.bfloat16)[None]
    partial_value = lax.psum_scatter(
        lax.dot_general(
            edge_inputs, cotangent, (((0,), (0,)), ((), ())), preferred_element_type=jnp.float32
        ),
        "rep",
        scatter_dimension=0,
        tiled=True,
    )
    weight_grad = lax.psum_scatter(partial_value, "sp", scatter_dimension=0, tiled=True)
    return (hidden, weight_grad)


OCTAVES = 40.0
LOWEST = 26.0
STEPS = 32767.0 / OCTAVES


def encode(value):
    level = (jnp.log2(jnp.maximum(jnp.abs(value), 2.0**-LOWEST)) + LOWEST) * STEPS
    code = jnp.minimum(level + 0.5, 32767.0).astype(jnp.int32)
    return jnp.where(value < 0, -code, code).astype(jnp.int16)


def decode(code):
    code = code.astype(jnp.int32)
    level = jnp.abs(code).astype(jnp.float32)
    size = jnp.exp2(level * (1.0 / STEPS) - LOWEST)
    return jnp.where(code > 0, size, jnp.where(code < 0, -size, 0.0))


def kernel(
    table_hbm, field_hbm, weights_hbm, edge_hbm, cot_hbm,
    hidden, grad,
    table, field, wide, weights, edge, cot, stage, outgoing, arrived, pool, tall,
    part, got1, link2, got2, link3, got3, linkz, gotz, linkf, gotf,
    load_sem, a2a_send, a2a_recv, s1, r1, s2, r2, s3, r3, sz, rz, sf, rf,
):
    rep = lax.axis_index("rep")
    me = lax.axis_index("sp")
    core = rep % 2
    x = (rep // 2) % 2
    y = rep // 4
    w1, w2 = 1 + core, 2 - core
    b1 = x + core * (y - x)
    b2 = y + core * (x - y)
    twin = rep + 1 - 2 * core
    first = rep + (1 - 2 * b1) * 2 * w1
    second = rep + (1 - 2 * b2) * 2 * w2
    low, high = me % 2, me // 2
    near = 2 * high + 1 - low
    far = 2 * (1 - high) + low
    diag = 2 * (1 - high) + 1 - low
    outer, inner = 3 * (1 - high), 2 - high
    channels, blocks, cells = field.shape
    pitch = wide.shape[1]
    tiles, reads, slots_each = hidden.shape[2], weights.shape[1], table.shape[1]
    width = edge_hbm.shape[1] // 4
    pieces = 2
    piece = slots_each // pieces

    loads = [
        pltpu.make_async_copy(field_hbm.at[0], field, load_sem.at[0]),
        pltpu.make_async_copy(table_hbm, table, load_sem.at[4]),
        pltpu.make_async_copy(edge_hbm, edge, load_sem.at[1]),
        pltpu.make_async_copy(cot_hbm, cot, load_sem.at[2]),
        pltpu.make_async_copy(weights_hbm, weights, load_sem.at[3]),
    ]
    for load in loads:
        load.start()
    field_load, table_load, edge_load, cot_load, weights_load = loads

    barrier = pltpu.get_barrier_semaphore()
    for peer in (far, diag, near):
        pl.semaphore_signal(barrier, inc=1, device_id=(rep, peer), device_id_type=MESH)
    for peer in (twin, first, second):
        pl.semaphore_signal(barrier, inc=1, device_id=(peer, me), device_id_type=MESH)

    field_load.wait()
    wide[:, :blocks, :] = field[...].astype(jnp.float32)
    rows = wide.reshape(channels * pitch, cells)
    table_load.wait()

    def block_for(d, j):
        block = rows[pl.ds(table[d, j], channels, stride=pitch), :]
        block = jnp.where(j < table[4 + tiles, d], block, jnp.zeros_like(block))
        return block

    def remote(src, dst, ssem, rsem, device):
        return pltpu.make_async_remote_copy(
            src_ref=src, dst_ref=dst, send_sem=ssem, recv_sem=rsem,
            device_id=device, device_id_type=MESH,
        )

    def send(*args):
        copy = remote(*args)
        copy.start()
        return copy

    end = (low + high) % 2 == 0
    middle = (low + high) % 2 == 1
    peers = (outer, near, inner)
    late = pieces - 1
    a2a = {}

    def choose(k, h):
        for n in range(piece):
            stage[pl.ds(n, channels, stride=piece), :] = block_for(peers[k], h * piece + n)
        outgoing[k, h] = stage[...].astype(outgoing.dtype)
        a2a[k, h] = remote(
            outgoing.at[k, h], arrived.at[me, h],
            a2a_send.at[k, h], a2a_recv.at[me, h], (rep, peers[k]),
        )

    def launch(where, keys):
        @pl.when(where)
        def _():
            for key in keys:
                a2a[key].start()

    for h in range(pieces):
        choose(0, h)
        if h == 0:
            pl.semaphore_wait(barrier, 6)
        a2a[0, h].start()
    for h in range(pieces):
        choose(2, h)
        if h < late:
            a2a[2, h].start()
        else:
            launch(end, [(2, h)])

    def chunk(flip1, flip2):
        return (b1 + flip1 * (1 - 2 * b1)) * w1 + (b2 + flip2 * (1 - 2 * b2)) * w2

    edge_load.wait()
    cot_load.wait()
    to_twin = []
    for k, (f1, f2) in enumerate(((1, 1), (0, 1), (1, 0), (0, 0))):
        q = chunk(f1, f2)
        columns = pl.ds(pl.multiple_of(q * width, 128), width)
        value = lax.dot_general(
            edge[:, columns], cot[...], (((0,), (0,)), ((), ())),
            preferred_element_type=jnp.float32,
        )
        part[k] = value.reshape(part.shape[1:])
        to_twin.append(send(
            part.at[k, 1 - core], got1.at[k], s1.at[k], r1.at[k], (twin, me)
        ))
    for h in range(pieces):
        choose(1, h)
    launch(middle, [(1, h) for h in range(pieces)])
    for j in range(slots_each):
        pool[me * slots_each + j] = block_for(me, j).astype(pool.dtype)

    order = [diag, near, far, me]
    both, crossed, after, kept = (0, 0), (2, 1), (1, 2), (3, 3)

    def folded(mine, theirs, i):
        return part[mine, core, order[i]] + got1[theirs, order[i]]

    out2, out3, outz = {}, {}, {}

    def hand_first(n, which, i):
        link2[n, i] = encode(folded(*which, i))
        out2[n, i] = send(
            link2.at[n, i], got2.at[n, i], s2.at[n, i], r2.at[n, i], (first, me)
        )

    def hand_second(i):
        value = folded(*after, i)
        out2[0, i].wait_recv()
        link3[i] = encode(value + decode(got2[0, i]))
        out3[i] = send(link3.at[i], got3.at[i], s3.at[i], r3.at[i], (second, me))

    def gathered(i):
        value = folded(*kept, i)
        out2[1, i].wait_recv()
        value = value + decode(got2[1, i])
        out3[i].wait_recv()
        return value + decode(got3[i])

    to_twin[both[1]].wait_recv()
    hand_first(0, both, 0)
    hand_first(0, both, 1)
    to_twin[crossed[1]].wait_recv()
    hand_first(1, crossed, 0)
    hand_first(1, crossed, 1)
    to_twin[after[1]].wait_recv()
    hand_second(0)
    hand_second(1)
    for i in (2, 3):
        hand_first(0, both, i)
        hand_first(1, crossed, i)
    to_twin[kept[1]].wait_recv()
    hand_second(2)
    hand_second(3)
    for i in (0, 1):
        linkz[i] = encode(gathered(i))
        outz[i] = send(linkz.at[i], gotz.at[i], sz.at[i], rz.at[i], (rep, near))
    for i in (2, 3):
        part[kept[0], core, order[i]] = gathered(i)
    launch(end, [(1, h) for h in range(pieces)])
    outz[0].wait_recv()
    linkf[...] = encode(part[kept[0], core, far] + decode(gotz[0]))
    last = send(linkf, gotf, sf, rf, (rep, far))
    launch(middle, [(2, h) for h in range(late, pieces)])
    outz[1].wait_recv()
    grad[...] = part[kept[0], core, me] + decode(gotz[1])

    weights_load.wait()
    for k, h in [(k, h) for k in range(3) for h in range(pieces)]:
        ready = arrived.at[peers[k], h]
        remote(
            ready, ready, a2a_send.at[k, h], a2a_recv.at[peers[k], h], (rep, peers[k])
        ).wait_recv()
        stage[...] = arrived[peers[k], h].astype(jnp.float32)
        for n in range(piece):
            block = stage[pl.ds(n, channels, stride=piece), :]
            pool[peers[k] * slots_each + h * piece + n] = block.astype(pool.dtype)
    for t in range(tiles):
        left = jnp.concatenate([pool[table[4 + t, b]] for b in range(reads)], axis=1)
        right = weights[t].reshape(reads * weights.shape[2], weights.shape[3])
        tall[pl.ds(t, channels, stride=tiles), :] = jnp.dot(
            left, right, preferred_element_type=jnp.float32
        )
    hidden[0] = tall[...].reshape(hidden.shape[1:]).astype(hidden.dtype)

    last.wait_recv()
    grad[...] = grad[...] + decode(gotf[...])
    for copies in (a2a, out2, out3, outz):
        for copy in copies.values():
            copy.wait_send()
    for copy in to_twin + [last]:
        copy.wait_send()


def settle(hidden, grad, hidden_out, grad_out, sem):
    pairs = ((hidden, hidden_out), (grad, grad_out))
    copies = [pltpu.make_async_copy(a, b, sem.at[i]) for i, (a, b) in enumerate(pairs)]
    for copy in copies:
        copy.start()
    for copy in copies:
        copy.wait()


def fused(field, send_blocks, send_count, regrid_weights, tile_slot, edge_inputs, cotangent):
    _, blocks, channels, cells = field.shape
    slots_each = send_blocks.shape[2]
    tiles = tile_slot.shape[0]
    nodes = regrid_weights.shape[3]
    n_in, hid = edge_inputs.shape[1], cotangent.shape[1]
    rows = n_in // (lax.axis_size("rep") * lax.axis_size("sp"))
    bf16, f32 = jnp.bfloat16, jnp.float32
    dma = pltpu.SemaphoreType.DMA
    i32, link = jnp.int32, jnp.int16
    far = pl.BlockSpec(memory_space=pl.ANY)
    near = pl.BlockSpec(memory_space=pltpu.VMEM)
    out_shape = (
        jax.ShapeDtypeStruct((1, channels, tiles, nodes), bf16),
        jax.ShapeDtypeStruct((rows, hid), f32),
    )
    shards = send_blocks.shape[1]
    width = max(slots_each, tile_slot.shape[1], shards)
    table = jnp.pad(send_blocks[0], ((0, tiles + 1), (0, width - slots_each)))
    table += jnp.pad(tile_slot, ((shards, 1), (0, width - tile_slot.shape[1])))
    table += jnp.pad(send_count, ((shards + tiles, 0), (0, width - shards)))
    hidden, grad = pl.pallas_call(
        kernel,
        out_shape=out_shape,
        in_specs=[far] * 5,
        out_specs=(near, near),
        scratch_shapes=[
            pltpu.SMEM(table.shape, i32),
            pltpu.VMEM((channels, blocks, cells), bf16),
            pltpu.VMEM((channels, blocks + 8, cells), f32),
            pltpu.VMEM(regrid_weights.shape, bf16),
            pltpu.VMEM(edge_inputs.shape, bf16),
            pltpu.VMEM(cotangent.shape, bf16),
            pltpu.VMEM((slots_each // 2 * channels, cells), f32),
            pltpu.VMEM((3, 2, slots_each // 2 * channels, cells), bf16),
            pltpu.VMEM((4, 2, slots_each // 2 * channels, cells), bf16),
            pltpu.VMEM((4 * slots_each, channels, cells), bf16),
            pltpu.VMEM((channels * tiles, nodes), f32),
            pltpu.VMEM((4, 2, 4, rows, hid), f32),
            pltpu.VMEM((4, 4, rows, hid), f32),
            pltpu.VMEM((2, 4, rows, hid), link),
            pltpu.VMEM((2, 4, rows, hid), link),
            pltpu.VMEM((4, rows, hid), link),
            pltpu.VMEM((4, rows, hid), link),
            pltpu.VMEM((2, rows, hid), link),
            pltpu.VMEM((2, rows, hid), link),
            pltpu.VMEM((rows, hid), link),
            pltpu.VMEM((rows, hid), link),
            dma((7,)),
            dma((3, 2)), dma((4, 2)),
            dma((4,)), dma((4,)),
            dma((2, 4)), dma((2, 4)),
            dma((4,)), dma((4,)),
            dma((2,)), dma((2,)),
            dma, dma,
        ],
        compiler_params=pltpu.CompilerParams(
            collective_id=0, has_side_effects=True, vmem_limit_bytes=56000000
        ),
    )(
        table, jnp.transpose(field, (0, 2, 1, 3)),
        regrid_weights, edge_inputs, cotangent,
    )
    hidden, grad = pl.pallas_call(
        settle, out_shape=out_shape, in_specs=[near, near], out_specs=(far, far),
        scratch_shapes=[dma((2,))],
        compiler_params=pltpu.CompilerParams(vmem_limit_bytes=2 * 1024 * 1024),
    )(hidden, grad)
    return jnp.transpose(hidden, (0, 2, 1, 3)), grad


def solution(mesh):
    in_specs = (
        P("rep", "sp", None, None),
        P("sp", None, None),
        P("sp", None),
        P("sp", None, None, None),
        P("sp", None),
        P(("rep", "sp"), None),
        P(("rep", "sp"), None),
    )
    out_specs = (P("rep", "sp", None, None), P(("rep", "sp"), None))
    binary = mesh.shape["rep"] == 2 * 2 * 2 and mesh.shape["sp"] == 2 * 2
    inner = fused if binary else body
    return jax.shard_map(inner, mesh=mesh, in_specs=in_specs, out_specs=out_specs, check_vma=False)
```

```python
import jax
import jax.numpy as jnp
from jax import lax
from jax.experimental import pallas as pl
from jax.experimental.pallas import tpu as pltpu
from jax.sharding import PartitionSpec as P

MESH = pl.DeviceIdType.MESH


def body(field, send_blocks, send_count, regrid_weights, tile_slot, edge_inputs, cotangent):
    sample = field[0]
    own_lists = send_blocks[0]
    shards = own_lists.shape[0]
    slots_each = own_lists.shape[1]
    channels = sample.shape[1]
    cells = sample.shape[2]
    alive = jnp.arange(slots_each, dtype=jnp.int32)[None, :] < send_count[0][:, None]
    outgoing = jnp.where(alive[:, :, None, None], sample[own_lists], jnp.zeros((), jnp.bfloat16))
    incoming = lax.all_to_all(outgoing, "sp", split_axis=0, concat_axis=0, tiled=True)
    block_pool = incoming.reshape(shards * slots_each, channels, cells)
    picked = block_pool[tile_slot]
    hidden = jnp.einsum(
        "tbcx,tbxn->tcn", picked, regrid_weights, preferred_element_type=jnp.float32
    )
    hidden = hidden.astype(jnp.bfloat16)[None]
    partial_value = lax.psum_scatter(
        lax.dot_general(
            edge_inputs, cotangent, (((0,), (0,)), ((), ())), preferred_element_type=jnp.float32
        ),
        "rep",
        scatter_dimension=0,
        tiled=True,
    )
    weight_grad = lax.psum_scatter(partial_value, "sp", scatter_dimension=0, tiled=True)
    return (hidden, weight_grad)


OCTAVES = 40.0
LOWEST = 26.0
STEPS = 32767.0 / OCTAVES


def encode(value):
    level = jnp.log2(jnp.abs(value)) * STEPS + (LOWEST * STEPS + 0.5)
    code = jnp.clip(level, 0.0, 32767.0).astype(jnp.int32)
    return jnp.where(value < 0, -code, code).astype(jnp.int16)


def decode(code):
    code = code.astype(jnp.int32)
    level = jnp.abs(code).astype(jnp.float32)
    size = jnp.exp2(level * (1.0 / STEPS) - LOWEST)
    return jnp.where(code > 0, size, jnp.where(code < 0, -size, 0.0))


def kernel(
    table_hbm, field_hbm, weights_hbm, edge_hbm, cot_hbm,
    hidden, grad,
    table, field, wide, weights, edge, cot, stage, outgoing, arrived, pool, tall,
    part, got1, link2, got2, link3, got3, linkz, gotz, linkf, gotf,
    load_sem, a2a_send, a2a_recv, s1, r1, s2, r2, s3, r3, sz, rz, sf, rf,
):
    rep = lax.axis_index("rep")
    me = lax.axis_index("sp")
    core = rep % 2
    x = (rep // 2) % 2
    y = rep // 4
    w1, w2 = 1 + core, 2 - core
    b1 = x + core * (y - x)
    b2 = y + core * (x - y)
    twin = rep + 1 - 2 * core
    first = rep + (1 - 2 * b1) * 2 * w1
    second = rep + (1 - 2 * b2) * 2 * w2
    low, high = me % 2, me // 2
    near = 2 * high + 1 - low
    far = 2 * (1 - high) + low
    diag = 2 * (1 - high) + 1 - low
    outer, inner = 3 * (1 - high), 2 - high
    channels, blocks, cells = field.shape
    pitch = wide.shape[1]
    tiles, reads = hidden.shape[2], weights.shape[1]
    width = edge_hbm.shape[1] // 4
    pieces = 2
    piece = stage.shape[0] // channels
    slots_each = piece * pieces

    loads = [
        pltpu.make_async_copy(field_hbm.at[0], field, load_sem.at[0]),
        pltpu.make_async_copy(table_hbm, table, load_sem.at[4]),
        pltpu.make_async_copy(edge_hbm, edge, load_sem.at[1]),
        pltpu.make_async_copy(cot_hbm, cot, load_sem.at[2]),
        pltpu.make_async_copy(weights_hbm, weights, load_sem.at[3]),
    ]
    for load in loads:
        load.start()
    field_load, table_load, edge_load, cot_load, weights_load = loads

    barrier = pltpu.get_barrier_semaphore()
    for peer in (far, diag, near):
        pl.semaphore_signal(barrier, inc=1, device_id=(rep, peer), device_id_type=MESH)
    for peer in (twin, first, second):
        pl.semaphore_signal(barrier, inc=1, device_id=(peer, me), device_id_type=MESH)

    field_load.wait()
    wide[:, :blocks, :] = field[...].astype(jnp.float32)
    rows = wide.reshape(channels * pitch, cells)
    table_load.wait()

    def block_for(d, j):
        block = rows[pl.ds(table[d, j], channels, stride=pitch), :]
        block = jnp.where(j < table[4 + tiles, d], block, jnp.zeros_like(block))
        return block

    def remote(src, dst, ssem, rsem, device):
        return pltpu.make_async_remote_copy(
            src_ref=src, dst_ref=dst, send_sem=ssem, recv_sem=rsem,
            device_id=device, device_id_type=MESH,
        )

    def send(*args):
        copy = remote(*args)
        copy.start()
        return copy

    end = (low + high) % 2 == 0
    middle = (low + high) % 2 == 1
    peers = (outer, near, inner)
    late = pieces - 1
    a2a = {}

    def choose(k, h):
        for n in range(piece):
            stage[pl.ds(n, channels, stride=piece), :] = block_for(peers[k], h * piece + n)
        outgoing[k, h] = stage[...].astype(outgoing.dtype)
        a2a[k, h] = remote(
            outgoing.at[k, h], arrived.at[me, h],
            a2a_send.at[k, h], a2a_recv.at[me, h], (rep, peers[k]),
        )

    def launch(where, keys):
        @pl.when(where)
        def _():
            for key in keys:
                a2a[key].start()

    for h in range(pieces):
        choose(0, h)
        if h == 0:
            pl.semaphore_wait(barrier, 6)
        a2a[0, h].start()
    for h in range(pieces):
        choose(2, h)
        if h < late:
            a2a[2, h].start()
        else:
            launch(end, [(2, h)])

    def chunk(flip1, flip2):
        return (b1 + flip1 * (1 - 2 * b1)) * w1 + (b2 + flip2 * (1 - 2 * b2)) * w2

    edge_load.wait()
    cot_load.wait()
    to_twin = []
    for k, (f1, f2) in enumerate(((1, 1), (0, 1), (1, 0), (0, 0))):
        q = chunk(f1, f2)
        columns = pl.ds(pl.multiple_of(q * width, 128), width)
        value = lax.dot_general(
            edge[:, columns], cot[...], (((0,), (0,)), ((), ())),
            preferred_element_type=jnp.float32,
        )
        part[k] = value.reshape(part.shape[1:])
        to_twin.append(send(
            part.at[k, 1 - core], got1.at[k], s1.at[k], r1.at[k], (twin, me)
        ))
    for h in range(pieces):
        choose(1, h)
    launch(middle, [(1, h) for h in range(pieces)])
    for j in range(slots_each):
        pool[me * slots_each + j] = block_for(me, j).astype(pool.dtype)

    order = [diag, near, far, me]
    both, crossed, after, kept = (0, 0), (2, 1), (1, 2), (3, 3)

    def folded(mine, theirs, i):
        return part[mine, core, order[i]] + got1[theirs, order[i]]

    out2, out3, outz = {}, {}, {}

    def hand_first(n, which, i):
        link2[n, i] = encode(folded(*which, i))
        out2[n, i] = send(
            link2.at[n, i], got2.at[n, i], s2.at[n, i], r2.at[n, i], (first, me)
        )

    def hand_second(i):
        value = folded(*after, i)
        out2[0, i].wait_recv()
        link3[i] = encode(value + decode(got2[0, i]))
        out3[i] = send(link3.at[i], got3.at[i], s3.at[i], r3.at[i], (second, me))

    def gathered(i):
        value = folded(*kept, i)
        out2[1, i].wait_recv()
        value = value + decode(got2[1, i])
        out3[i].wait_recv()
        return value + decode(got3[i])

    to_twin[both[1]].wait_recv()
    hand_first(0, both, 0)
    hand_first(0, both, 1)
    to_twin[crossed[1]].wait_recv()
    hand_first(1, crossed, 0)
    hand_first(1, crossed, 1)
    for i in (2, 3):
        hand_first(0, both, i)
        hand_first(1, crossed, i)
    to_twin[after[1]].wait_recv()
    hand_second(0)
    hand_second(1)
    to_twin[kept[1]].wait_recv()
    hand_second(2)
    hand_second(3)
    for i in (0, 1):
        linkz[i] = encode(gathered(i))
        outz[i] = send(linkz.at[i], gotz.at[i], sz.at[i], rz.at[i], (rep, near))
    for i in (2, 3):
        part[kept[0], core, order[i]] = gathered(i)
    launch(end, [(1, h) for h in range(pieces)])
    outz[0].wait_recv()
    linkf[...] = encode(part[kept[0], core, far] + decode(gotz[0]))
    last = send(linkf, gotf, sf, rf, (rep, far))
    launch(middle, [(2, h) for h in range(late, pieces)])
    outz[1].wait_recv()
    grad[...] = part[kept[0], core, me] + decode(gotz[1])

    weights_load.wait()
    for k, h in [(k, h) for k in range(3) for h in range(pieces)]:
        ready = arrived.at[peers[k], h]
        remote(
            ready, ready, a2a_send.at[k, h], a2a_recv.at[peers[k], h], (rep, peers[k])
        ).wait_recv()
        stage[...] = arrived[peers[k], h].astype(jnp.float32)
        for n in range(piece):
            block = stage[pl.ds(n, channels, stride=piece), :]
            pool[peers[k] * slots_each + h * piece + n] = block.astype(pool.dtype)
    for t in range(tiles):
        left = jnp.concatenate([pool[table[4 + t, b]] for b in range(reads)], axis=1)
        right = weights[t].reshape(reads * weights.shape[2], weights.shape[3])
        tall[pl.ds(t, channels, stride=tiles), :] = jnp.dot(
            left, right, preferred_element_type=jnp.float32
        )
    hidden[0] = tall[...].reshape(hidden.shape[1:]).astype(hidden.dtype)

    last.wait_recv()
    grad[...] = grad[...] + decode(gotf[...])
    for copies in (a2a, out2, out3, outz):
        for copy in copies.values():
            copy.wait_send()
    for copy in to_twin + [last]:
        copy.wait_send()


def settle(hidden, grad, hidden_out, grad_out, sem):
    pairs = ((hidden, hidden_out), (grad, grad_out))
    copies = [pltpu.make_async_copy(a, b, sem.at[i]) for i, (a, b) in enumerate(pairs)]
    for copy in copies:
        copy.start()
    for copy in copies:
        copy.wait()


def fused(field, send_blocks, send_count, regrid_weights, tile_slot, edge_inputs, cotangent):
    _, blocks, channels, cells = field.shape
    slots_each = send_blocks.shape[2]
    tiles = tile_slot.shape[0]
    nodes = regrid_weights.shape[3]
    n_in, hid = edge_inputs.shape[1], cotangent.shape[1]
    rows = n_in // (lax.axis_size("rep") * lax.axis_size("sp"))
    bf16, f32 = jnp.bfloat16, jnp.float32
    dma = pltpu.SemaphoreType.DMA
    i32, link = jnp.int32, jnp.int16
    far = pl.BlockSpec(memory_space=pl.ANY)
    near = pl.BlockSpec(memory_space=pltpu.VMEM)
    out_shape = (
        jax.ShapeDtypeStruct((1, channels, tiles, nodes), bf16),
        jax.ShapeDtypeStruct((rows, hid), f32),
    )
    shards = send_blocks.shape[1]
    width = max(slots_each, tile_slot.shape[1], shards)
    table = jnp.pad(send_blocks[0], ((0, tiles + 1), (0, width - slots_each)))
    table += jnp.pad(tile_slot, ((shards, 1), (0, width - tile_slot.shape[1])))
    table += jnp.pad(send_count, ((shards + tiles, 0), (0, width - shards)))
    hidden, grad = pl.pallas_call(
        kernel,
        out_shape=out_shape,
        in_specs=[far] * 5,
        out_specs=(near, near),
        scratch_shapes=[
            pltpu.SMEM(table.shape, i32),
            pltpu.VMEM((channels, blocks, cells), bf16),
            pltpu.VMEM((channels, blocks + 8, cells), f32),
            pltpu.VMEM(regrid_weights.shape, bf16),
            pltpu.VMEM(edge_inputs.shape, bf16),
            pltpu.VMEM(cotangent.shape, bf16),
            pltpu.VMEM((slots_each // 2 * channels, cells), f32),
            pltpu.VMEM((3, 2, slots_each // 2 * channels, cells), bf16),
            pltpu.VMEM((4, 2, slots_each // 2 * channels, cells), bf16),
            pltpu.VMEM((4 * slots_each, channels, cells), bf16),
            pltpu.VMEM((channels * tiles, nodes), f32),
            pltpu.VMEM((4, 2, 4, rows, hid), f32),
            pltpu.VMEM((4, 4, rows, hid), f32),
            pltpu.VMEM((2, 4, rows, hid), link),
            pltpu.VMEM((2, 4, rows, hid), link),
            pltpu.VMEM((4, rows, hid), link),
            pltpu.VMEM((4, rows, hid), link),
            pltpu.VMEM((2, rows, hid), link),
            pltpu.VMEM((2, rows, hid), link),
            pltpu.VMEM((rows, hid), link),
            pltpu.VMEM((rows, hid), link),
            dma((7,)),
            dma((3, 2)), dma((4, 2)),
            dma((4,)), dma((4,)),
            dma((2, 4)), dma((2, 4)),
            dma((4,)), dma((4,)),
            dma((2,)), dma((2,)),
            dma, dma,
        ],
        compiler_params=pltpu.CompilerParams(
            collective_id=0, has_side_effects=True, vmem_limit_bytes=56000000
        ),
    )(
        table, jnp.transpose(field, (0, 2, 1, 3)),
        regrid_weights, edge_inputs, cotangent,
    )
    hidden, grad = pl.pallas_call(
        settle, out_shape=out_shape, in_specs=[near, near], out_specs=(far, far),
        scratch_shapes=[dma((2,))],
        compiler_params=pltpu.CompilerParams(vmem_limit_bytes=2 * 1024 * 1024),
    )(hidden, grad)
    return jnp.transpose(hidden, (0, 2, 1, 3)), grad


def solution(mesh):
    in_specs = (
        P("rep", "sp", None, None),
        P("sp", None, None),
        P("sp", None),
        P("sp", None, None, None),
        P("sp", None),
        P(("rep", "sp"), None),
        P(("rep", "sp"), None),
    )
    out_specs = (P("rep", "sp", None, None), P(("rep", "sp"), None))
    binary = mesh.shape["rep"] == 2 * 2 * 2 and mesh.shape["sp"] == 2 * 2
    inner = fused if binary else body
    return jax.shard_map(inner, mesh=mesh, in_specs=in_specs, out_specs=out_specs, check_vma=False)
```

```python
import jax
import jax.numpy as jnp
from jax import lax
from jax.experimental import pallas as pl
from jax.experimental.pallas import tpu as pltpu
from jax.sharding import PartitionSpec as P

MESH = pl.DeviceIdType.MESH


def body(field, send_blocks, send_count, regrid_weights, tile_slot, edge_inputs, cotangent):
    sample = field[0]
    own_lists = send_blocks[0]
    shards = own_lists.shape[0]
    slots_each = own_lists.shape[1]
    channels = sample.shape[1]
    cells = sample.shape[2]
    alive = jnp.arange(slots_each, dtype=jnp.int32)[None, :] < send_count[0][:, None]
    outgoing = jnp.where(alive[:, :, None, None], sample[own_lists], jnp.zeros((), jnp.bfloat16))
    incoming = lax.all_to_all(outgoing, "sp", split_axis=0, concat_axis=0, tiled=True)
    block_pool = incoming.reshape(shards * slots_each, channels, cells)
    picked = block_pool[tile_slot]
    hidden = jnp.einsum(
        "tbcx,tbxn->tcn", picked, regrid_weights, preferred_element_type=jnp.float32
    )
    hidden = hidden.astype(jnp.bfloat16)[None]
    partial_value = lax.psum_scatter(
        lax.dot_general(
            edge_inputs, cotangent, (((0,), (0,)), ((), ())), preferred_element_type=jnp.float32
        ),
        "rep",
        scatter_dimension=0,
        tiled=True,
    )
    weight_grad = lax.psum_scatter(partial_value, "sp", scatter_dimension=0, tiled=True)
    return (hidden, weight_grad)


OCTAVES = 40.0
LOWEST = 26.0
STEPS = 32767.0 / OCTAVES


def encode(value):
    level = jnp.log2(jnp.abs(value)) * STEPS + (LOWEST * STEPS + 0.5)
    code = jnp.clip(level, 0.0, 32767.0).astype(jnp.int32)
    return jnp.where(value < 0, -code, code).astype(jnp.int16)


def decode(code):
    code = code.astype(jnp.int32)
    level = jnp.abs(code).astype(jnp.float32)
    size = jnp.exp2(level * (1.0 / STEPS) - LOWEST)
    return jnp.where(code > 0, size, jnp.where(code < 0, -size, 0.0))


def kernel(
    table_hbm, field_hbm, weights_hbm, edge_hbm, cot_hbm,
    hidden, grad,
    table, field, wide, weights, edge, cot, stage, outgoing, arrived, pool, tall,
    part, got1, link2, got2, link3, got3, linkz, gotz, linkf, gotf,
    load_sem, a2a_send, a2a_recv, s1, r1, s2, r2, s3, r3, sz, rz, sf, rf, ready,
):
    rep = lax.axis_index("rep")
    me = lax.axis_index("sp")
    core = rep % 2
    x = (rep // 2) % 2
    y = rep // 4
    w1, w2 = 1 + core, 2 - core
    b1 = x + core * (y - x)
    b2 = y + core * (x - y)
    twin = rep + 1 - 2 * core
    first = rep + (1 - 2 * b1) * 2 * w1
    second = rep + (1 - 2 * b2) * 2 * w2
    low, high = me % 2, me // 2
    near = 2 * high + 1 - low
    far = 2 * (1 - high) + low
    diag = 2 * (1 - high) + 1 - low
    ahead, behind = 2 * (1 - high), 3 - 2 * high
    last_shard = me == 3
    channels, blocks, cells = field.shape
    pitch = wide.shape[1]
    tiles, reads = hidden.shape[2], weights.shape[1]
    width = edge_hbm.shape[1] // 4
    pieces = 2
    piece = stage.shape[0] // channels
    slots_each = piece * pieces

    loads = [
        pltpu.make_async_copy(field_hbm.at[0], field, load_sem.at[0]),
        pltpu.make_async_copy(table_hbm, table, load_sem.at[4]),
        pltpu.make_async_copy(edge_hbm, edge, load_sem.at[1]),
        pltpu.make_async_copy(cot_hbm, cot, load_sem.at[2]),
        pltpu.make_async_copy(weights_hbm, weights, load_sem.at[3]),
    ]
    for load in loads:
        load.start()
    field_load, table_load, edge_load, cot_load, weights_load = loads

    barrier = pltpu.get_barrier_semaphore()
    @pl.when(jnp.logical_not(last_shard))
    def _():
        for peer in (far, diag, near):
            pl.semaphore_signal(barrier, inc=1, device_id=(rep, peer), device_id_type=MESH)

    for peer in (twin, first, second):
        pl.semaphore_signal(barrier, inc=1, device_id=(peer, me), device_id_type=MESH)

    field_load.wait()
    wide[:, :blocks, :] = field[...].astype(jnp.float32)
    rows = wide.reshape(channels * pitch, cells)
    table_load.wait()

    def block_for(d, j):
        block = rows[pl.ds(table[d, j], channels, stride=pitch), :]
        block = jnp.where(j < table[4 + tiles, d], block, jnp.zeros_like(block))
        return block

    def remote(src, dst, ssem, rsem, device):
        return pltpu.make_async_remote_copy(
            src_ref=src, dst_ref=dst, send_sem=ssem, recv_sem=rsem,
            device_id=device, device_id_type=MESH,
        )

    def send(*args):
        copy = remote(*args)
        copy.start()
        return copy

    end = (low + high) % 2 == 0
    middle = (low + high) % 2 == 1
    upper, lower = high == 1, high == 0
    peers = (ahead, near, behind)
    a2a = {}

    def choose(k, h):
        for n in range(piece):
            stage[pl.ds(n, channels, stride=piece), :] = block_for(peers[k], h * piece + n)
        outgoing[k, h] = stage[...].astype(outgoing.dtype)
        a2a[k, h] = remote(
            outgoing.at[k, h], arrived.at[me, h],
            a2a_send.at[k, h], a2a_recv.at[me, h], (rep, peers[k]),
        )

    def launch(where, keys):
        @pl.when(where)
        def _():
            for key in keys:
                a2a[key].start()

    choose(0, 0)
    pl.semaphore_wait(barrier, 5 + me // 3)

    @pl.when(last_shard)
    def _():
        for peer in (far, diag, near):
            pl.semaphore_signal(ready, inc=1, device_id=(rep, peer), device_id_type=MESH)

    a2a[0, 0].start()
    choose(0, 1)
    a2a[0, 1].start()
    choose(2, 0)
    launch(upper, [(2, 0)])
    choose(2, 1)
    launch(last_shard & (core == 0), [(2, 1)])

    def chunk(flip1, flip2):
        return (b1 + flip1 * (1 - 2 * b1)) * w1 + (b2 + flip2 * (1 - 2 * b2)) * w2

    edge_load.wait()
    cot_load.wait()
    to_twin = []
    for k, (f1, f2) in enumerate(((1, 1), (0, 1), (1, 0), (0, 0))):
        q = chunk(f1, f2)
        columns = pl.ds(pl.multiple_of(q * width, 128), width)
        value = lax.dot_general(
            edge[:, columns], cot[...], (((0,), (0,)), ((), ())),
            preferred_element_type=jnp.float32,
        )
        part[k] = value.reshape(part.shape[1:])
        to_twin.append(send(
            part.at[k, 1 - core], got1.at[k], s1.at[k], r1.at[k], (twin, me)
        ))
    for h in range(pieces):
        choose(1, h)
    launch(middle & lower, [(1, h) for h in range(pieces)])
    for j in range(slots_each):
        pool[me * slots_each + j] = block_for(me, j).astype(pool.dtype)

    order = [diag, near, far, me]
    both, crossed, after, kept = (0, 0), (2, 1), (1, 2), (3, 3)

    def folded(mine, theirs, i):
        return part[mine, core, order[i]] + got1[theirs, order[i]]

    out2, out3, outz = {}, {}, {}

    def hand_first(n, which, i):
        link2[n, i] = encode(folded(*which, i))
        out2[n, i] = send(
            link2.at[n, i], got2.at[n, i], s2.at[n, i], r2.at[n, i], (first, me)
        )

    def hand_second(i):
        value = folded(*after, i)
        out2[0, i].wait_recv()
        link3[i] = encode(value + decode(got2[0, i]))
        out3[i] = send(link3.at[i], got3.at[i], s3.at[i], r3.at[i], (second, me))

    def gathered(i):
        value = folded(*kept, i)
        out2[1, i].wait_recv()
        value = value + decode(got2[1, i])
        out3[i].wait_recv()
        return value + decode(got3[i])

    @pl.when(jnp.logical_not(last_shard))
    def _():
        pl.semaphore_wait(ready, 1)

    launch(lower, [(2, 0)])
    launch(end & lower, [(2, 1)])
    launch(middle & upper, [(1, h) for h in range(pieces)])
    to_twin[both[1]].wait_recv()
    hand_first(0, both, 0)
    hand_first(0, both, 1)
    to_twin[crossed[1]].wait_recv()
    hand_first(1, crossed, 0)
    hand_first(1, crossed, 1)
    for i in (2, 3):
        hand_first(0, both, i)
        hand_first(1, crossed, i)
    to_twin[after[1]].wait_recv()
    hand_second(0)
    hand_second(1)
    to_twin[kept[1]].wait_recv()
    hand_second(2)
    hand_second(3)
    for i in (0, 1):
        linkz[i] = encode(gathered(i))
        outz[i] = send(linkz.at[i], gotz.at[i], sz.at[i], rz.at[i], (rep, near))
    for i in (2, 3):
        part[kept[0], core, order[i]] = gathered(i)
    launch(last_shard & (core == 1), [(2, 1)])
    launch(end, [(1, h) for h in range(pieces)])
    outz[0].wait_recv()
    linkf[...] = encode(part[kept[0], core, far] + decode(gotz[0]))
    last = send(linkf, gotf, sf, rf, (rep, far))
    launch(middle & upper, [(2, 1)])
    launch(middle & lower, [(2, 1)])
    outz[1].wait_recv()
    grad[...] = part[kept[0], core, me] + decode(gotz[1])

    weights_load.wait()
    for k, h in [(k, h) for k in range(3) for h in range(pieces)]:
        ready = arrived.at[peers[k], h]
        remote(
            ready, ready, a2a_send.at[k, h], a2a_recv.at[peers[k], h], (rep, peers[k])
        ).wait_recv()
        stage[...] = arrived[peers[k], h].astype(jnp.float32)
        for n in range(piece):
            block = stage[pl.ds(n, channels, stride=piece), :]
            pool[peers[k] * slots_each + h * piece + n] = block.astype(pool.dtype)
    for t in range(tiles):
        left = jnp.concatenate([pool[table[4 + t, b]] for b in range(reads)], axis=1)
        right = weights[t].reshape(reads * weights.shape[2], weights.shape[3])
        tall[pl.ds(t, channels, stride=tiles), :] = jnp.dot(
            left, right, preferred_element_type=jnp.float32
        )
    hidden[0] = tall[...].reshape(hidden.shape[1:]).astype(hidden.dtype)

    last.wait_recv()
    grad[...] = grad[...] + decode(gotf[...])
    for copies in (a2a, out2, out3, outz):
        for copy in copies.values():
            copy.wait_send()
    for copy in to_twin + [last]:
        copy.wait_send()


def settle(hidden, grad, hidden_out, grad_out, sem):
    pairs = ((hidden, hidden_out), (grad, grad_out))
    copies = [pltpu.make_async_copy(a, b, sem.at[i]) for i, (a, b) in enumerate(pairs)]
    for copy in copies:
        copy.start()
    for copy in copies:
        copy.wait()


def fused(field, send_blocks, send_count, regrid_weights, tile_slot, edge_inputs, cotangent):
    _, blocks, channels, cells = field.shape
    slots_each = send_blocks.shape[2]
    tiles = tile_slot.shape[0]
    nodes = regrid_weights.shape[3]
    n_in, hid = edge_inputs.shape[1], cotangent.shape[1]
    rows = n_in // (lax.axis_size("rep") * lax.axis_size("sp"))
    bf16, f32 = jnp.bfloat16, jnp.float32
    dma = pltpu.SemaphoreType.DMA
    i32, link = jnp.int32, jnp.int16
    far = pl.BlockSpec(memory_space=pl.ANY)
    near = pl.BlockSpec(memory_space=pltpu.VMEM)
    out_shape = (
        jax.ShapeDtypeStruct((1, channels, tiles, nodes), bf16),
        jax.ShapeDtypeStruct((rows, hid), f32),
    )
    shards = send_blocks.shape[1]
    width = max(slots_each, tile_slot.shape[1], shards)
    table = jnp.pad(send_blocks[0], ((0, tiles + 1), (0, width - slots_each)))
    table += jnp.pad(tile_slot, ((shards, 1), (0, width - tile_slot.shape[1])))
    table += jnp.pad(send_count, ((shards + tiles, 0), (0, width - shards)))
    hidden, grad = pl.pallas_call(
        kernel,
        out_shape=out_shape,
        in_specs=[far] * 5,
        out_specs=(near, near),
        scratch_shapes=[
            pltpu.SMEM(table.shape, i32),
            pltpu.VMEM((channels, blocks, cells), bf16),
            pltpu.VMEM((channels, blocks + 8, cells), f32),
            pltpu.VMEM(regrid_weights.shape, bf16),
            pltpu.VMEM(edge_inputs.shape, bf16),
            pltpu.VMEM(cotangent.shape, bf16),
            pltpu.VMEM((slots_each // 2 * channels, cells), f32),
            pltpu.VMEM((3, 2, slots_each // 2 * channels, cells), bf16),
            pltpu.VMEM((4, 2, slots_each // 2 * channels, cells), bf16),
            pltpu.VMEM((4 * slots_each, channels, cells), bf16),
            pltpu.VMEM((channels * tiles, nodes), f32),
            pltpu.VMEM((4, 2, 4, rows, hid), f32),
            pltpu.VMEM((4, 4, rows, hid), f32),
            pltpu.VMEM((2, 4, rows, hid), link),
            pltpu.VMEM((2, 4, rows, hid), link),
            pltpu.VMEM((4, rows, hid), link),
            pltpu.VMEM((4, rows, hid), link),
            pltpu.VMEM((2, rows, hid), link),
            pltpu.VMEM((2, rows, hid), link),
            pltpu.VMEM((rows, hid), link),
            pltpu.VMEM((rows, hid), link),
            dma((7,)),
            dma((3, 2)), dma((4, 2)),
            dma((4,)), dma((4,)),
            dma((2, 4)), dma((2, 4)),
            dma((4,)), dma((4,)),
            dma((2,)), dma((2,)),
            dma, dma,
            pltpu.SemaphoreType.REGULAR,
        ],
        compiler_params=pltpu.CompilerParams(
            collective_id=0, has_side_effects=True, vmem_limit_bytes=56000000
        ),
    )(
        table, jnp.transpose(field, (0, 2, 1, 3)),
        regrid_weights, edge_inputs, cotangent,
    )
    hidden, grad = pl.pallas_call(
        settle, out_shape=out_shape, in_specs=[near, near], out_specs=(far, far),
        scratch_shapes=[dma((2,))],
        compiler_params=pltpu.CompilerParams(vmem_limit_bytes=2 * 1024 * 1024),
    )(hidden, grad)
    return jnp.transpose(hidden, (0, 2, 1, 3)), grad


def solution(mesh):
    in_specs = (
        P("rep", "sp", None, None),
        P("sp", None, None),
        P("sp", None),
        P("sp", None, None, None),
        P("sp", None),
        P(("rep", "sp"), None),
        P(("rep", "sp"), None),
    )
    out_specs = (P("rep", "sp", None, None), P(("rep", "sp"), None))
    binary = mesh.shape["rep"] == 2 * 2 * 2 and mesh.shape["sp"] == 2 * 2
    inner = fused if binary else body
    return jax.shard_map(inner, mesh=mesh, in_specs=in_specs, out_specs=out_specs, check_vma=False)
```
